256 devices in a mesh: tm: 16 (over x, y), paths: 16 (over z, core).
Axes of the slice: x: 4, y: 4, z: 8, core: 2. Of those that a mesh axis runs over, the one named last changes fastest.
Arguments:
- returns: bfloat16 [512, 8192, 256], P('tm', 'paths'), may hold values from -0.15917969 to 0.15917969
- weights: bfloat16 [256, 64], P('paths'), may hold values from -0.375 to 0.375
Outputs:
- drawdown: float32 [64, 8192], P('tm', 'paths')
The draws below stay inside these ranges and needn't reach their ends.
All inputs are finite; a program needn't handle non-finite values.
Results may differ from the reference program's by a relative error of at most 0.0003.
Values may be sent and summed in bfloat16 or wider, within the bound.
A program may use at most 64 MiB of HBM per device.

```python
import jax
import jax.numpy as jnp
from jax import lax

ASSETS = 256
PORT = 64
T_DEV = 32
STEPS = 512
PATHS = 8192
N_TM = 16


def block_levels(key, shape, shards, smallest, high):
    loudness = 1.0
    for dim, parts in shards:
        heights = jax.random.uniform(jax.random.fold_in(jax.random.fold_in(key, 6), dim), (parts,), jnp.float32, smallest / len(shards), high / len(shards))
        loudness = loudness * jnp.repeat(jnp.exp(heights), shape[dim] // parts).reshape((-1,) + (1,) * (len(shape) - 1 - dim))
    return loudness


def bell_draw(stream_key, dims, spread, limit, split=(), kind=jnp.bfloat16):
    loudness = block_levels(stream_key, dims, split, -0.22, 0.18) if split else 1.0
    array = jax.random.normal(stream_key, dims, jnp.float32) * spread * loudness
    return jnp.minimum(jnp.maximum(array, -limit), limit).astype(kind)


def setup_inputs(seed: int = 0) -> dict:
    keys = jax.random.split(jax.random.key(seed), 3)
    return {
        "returns": bell_draw(keys[0], (STEPS, PATHS, ASSETS), 0.02, 0.15917969, ((0, 16), (1, 16))),
        "weights": bell_draw(keys[1], (ASSETS, PORT), ASSETS ** -0.5, 0.375, ((0, 16),)),
    }


def reference(returns, weights):
    blocks = returns.reshape(N_TM, T_DEV, PATHS, ASSETS)
    holdings = weights.astype(jnp.float32)

    def advance(carry, block):
        level, highest, deepest = carry
        profit = jnp.einsum('tpa,aq->tqp', block.astype(jnp.float32), holdings)
        value = level[None] + jnp.cumsum(profit, axis=0)
        running = jnp.maximum(highest[None], lax.cummax(value, axis=0))
        deepest = jnp.maximum(deepest, jnp.max(running - value, axis=0))
        return (value[-1], running[-1], deepest), None

    zeros = jnp.zeros((PORT, PATHS), jnp.float32)
    final, unused = lax.scan(advance, (zeros, zeros, zeros), blocks)
    return final[2]
```

```python
import jax
import jax.numpy as jnp
from jax import lax
from jax.experimental import pallas as pl
from jax.experimental.pallas import tpu as pltpu
from jax.sharding import PartitionSpec as P

MESH = pl.DeviceIdType.MESH
LANES = 128
SUB = 8


def kernel(n_tm, n_paths, ret_ref, w_ref, out_ref,
           x, w_in, w_all, y, outbox, inbox,
           x_sem, w_in_sem, w_send_sem, w_recv_sem, send_sem, recv_sem):
    tm = lax.axis_index("tm")
    paths = lax.axis_index("paths")
    steps, n_local, assets = ret_ref.shape
    rows, port = w_ref.shape
    chunks = n_local // LANES
    half = steps // 2
    held = port // n_tm

    barrier = pltpu.get_barrier_semaphore()
    for d in range(1, n_paths):
        pl.semaphore_signal(barrier, inc=1, device_id=(tm, lax.rem(paths + d, n_paths)), device_id_type=MESH)
    for d in range(1, n_tm):
        pl.semaphore_signal(barrier, inc=1, device_id=(lax.rem(tm + d, n_tm), paths), device_id_type=MESH)
    w_load = pltpu.make_async_copy(w_ref, w_in, w_in_sem)
    w_load.start()
    loads = []
    for c in range(chunks):
        load = pltpu.make_async_copy(ret_ref.at[:, pl.ds(c * LANES, LANES), :], x.at[c], x_sem.at[c])
        load.start()
        loads.append(load)

    w_load.wait()
    source = lax.broadcasted_iota(jnp.int32, (port, LANES), 0)
    lane = lax.broadcasted_iota(jnp.int32, (port, LANES), 1)
    spread = jnp.where(source == (lane // SUB) * held + lane % held, 1.0, 0.0).astype(jnp.bfloat16)
    own_rows = pl.ds(pl.multiple_of(paths * rows, rows), rows)
    w_all[own_rows, :] = jnp.dot(w_in[...], spread, preferred_element_type=jnp.float32).astype(jnp.bfloat16)

    pl.semaphore_wait(barrier, n_paths - 1 + n_tm - 1)

    w_sends = []
    order = sorted(range(1, n_paths), key=lambda d: -min(d, n_paths - d))
    for d in order:
        copy = pltpu.make_async_remote_copy(
            src_ref=w_all.at[own_rows, :], dst_ref=w_all.at[own_rows, :],
            send_sem=w_send_sem.at[d], recv_sem=w_recv_sem.at[d],
            device_id=(tm, lax.rem(paths + d, n_paths)), device_id_type=MESH)
        copy.start()
        w_sends.append(copy)
    for copy in reversed(w_sends):
        copy.wait_recv()

    lane_w = lax.broadcasted_iota(jnp.int32, (assets, LANES), 1)
    first = (lane_w % SUB) < held
    w_all_now = w_all[...].astype(jnp.float32)
    w_a = jnp.where(first, w_all_now, 0.0).astype(jnp.bfloat16)
    w_b = jnp.where(first, 0.0, w_all_now).astype(jnp.bfloat16)

    second = (lax.broadcasted_iota(jnp.int32, (LANES, LANES), 1) % SUB) >= held
    tm_order = list(range(1, n_tm))
    sends = []
    for c in range(chunks):
        loads[c].wait()
        x_a = x[c, 0:half].reshape(half * LANES, assets)
        x_b = x[c, half:steps].reshape(half * LANES, assets)
        y[...] = (jnp.dot(x_a, w_a, preferred_element_type=jnp.float32)
                  + jnp.dot(x_b, w_b, preferred_element_type=jnp.float32))
        total, high, low, deep = [], [], [], []
        for r in range(0, LANES, 32):
            v = y[pl.ds(r, 32), :]
            hi = jnp.maximum(v, 0.0)
            lo = jnp.minimum(v, 0.0)
            dd = hi - v
            for t in range(1, half):
                v = v + y[pl.ds(t * LANES + r, 32), :]
                hi = jnp.maximum(hi, v)
                lo = jnp.minimum(lo, v)
                dd = jnp.maximum(dd, hi - v)
            total.append(v)
            high.append(hi)
            low.append(lo)
            deep.append(dd)
        total, high, low, deep = (jnp.concatenate(part, axis=0) for part in (total, high, low, deep))
        t0, h0, l0, d0 = (pltpu.roll(part, held, 1) for part in (total, high, low, deep))
        m_total = t0 + total
        m_high = jnp.maximum(h0, t0 + high)
        m_low = jnp.minimum(l0, t0 + low)
        m_deep = jnp.maximum(jnp.maximum(d0, deep), h0 - (t0 + low))
        th = jnp.where(second, m_high, pltpu.roll(m_total, LANES - held, 1))
        ld = jnp.where(second, m_deep, pltpu.roll(m_low, LANES - held, 1))
        outbox[c, :, 0] = th.T.reshape(n_tm, SUB, LANES)
        outbox[c, :, 1] = ld.T.reshape(n_tm, SUB, LANES)
        for d in tm_order:
            to = lax.rem(tm + d, n_tm)
            copy = pltpu.make_async_remote_copy(
                src_ref=outbox.at[c, to], dst_ref=inbox.at[c, tm],
                send_sem=send_sem.at[c, d], recv_sem=recv_sem.at[c, d],
                device_id=(to, paths), device_id_type=MESH)
            copy.start()
            sends.append(copy)
        inbox[c, pl.ds(tm, 1)] = outbox[c, pl.ds(tm, 1)]

    for c in range(chunks):
        for copy in sends[c * len(tm_order):(c + 1) * len(tm_order)]:
            copy.wait_recv()
        offset = jnp.zeros((SUB, LANES), jnp.float32)
        peak = jnp.zeros((SUB, LANES), jnp.float32)
        fall = jnp.zeros((SUB, LANES), jnp.float32)
        for s in range(n_tm):
            th = inbox[c, s, 0]
            ld = inbox[c, s, 1]
            fall = jnp.maximum(fall, jnp.maximum(pltpu.roll(ld, held, 0), peak - (offset + ld)))
            peak = jnp.maximum(peak, offset + pltpu.roll(th, held, 0))
            offset = offset + th
        out_ref[:, pl.ds(c * LANES, LANES)] = fall[:held]

    for copy in w_sends:
        copy.wait_send()
    for copy in sends:
        copy.wait_send()


def shards(returns, weights):
    n_tm, n_paths = lax.axis_size("tm"), lax.axis_size("paths")
    steps, n_local, assets = returns.shape
    rows, port = weights.shape
    chunks = n_local // LANES
    half = steps // 2
    held = port // n_tm
    f32 = jnp.float32
    return pl.pallas_call(
        lambda *refs: kernel(n_tm, n_paths, *refs),
        name="drawdown",
        out_shape=jax.ShapeDtypeStruct((held, n_local), f32),
        in_specs=[pl.BlockSpec(memory_space=pltpu.HBM)] * 2,
        out_specs=pl.BlockSpec(memory_space=pltpu.VMEM),
        scratch_shapes=[
            pltpu.VMEM((chunks, steps, LANES, assets), jnp.bfloat16),
            pltpu.VMEM((rows, port), jnp.bfloat16),
            pltpu.VMEM((assets, LANES), jnp.bfloat16),
            pltpu.VMEM((half * LANES, LANES), f32),
            pltpu.VMEM((chunks, n_tm, 2, SUB, LANES), f32),
            pltpu.VMEM((chunks, n_tm, 2, SUB, LANES), f32),
            pltpu.SemaphoreType.DMA((chunks,)),
            pltpu.SemaphoreType.DMA,
            pltpu.SemaphoreType.DMA((n_paths,)),
            pltpu.SemaphoreType.DMA((n_paths,)),
            pltpu.SemaphoreType.DMA((chunks, n_tm)),
            pltpu.SemaphoreType.DMA((chunks, n_tm)),
        ],
        compiler_params=pltpu.CompilerParams(
            collective_id=0, has_side_effects=True, vmem_limit_bytes=67043328
        ),
    )(returns, weights)


def solution(mesh):
    in_specs = (P("tm", "paths", None), P("paths", None))
    out_specs = P("tm", "paths")
    return jax.shard_map(shards, mesh=mesh, in_specs=in_specs, out_specs=out_specs, check_vma=False)
```

```python
import jax
import jax.numpy as jnp
from jax import lax
from jax.experimental import pallas as pl
from jax.experimental.pallas import tpu as pltpu
from jax.sharding import PartitionSpec as P

MESH = pl.DeviceIdType.MESH
LANES = 128
SUB = 8
SIDE = 4
PAIR = 2
HOPS = sorted(
    ((dx, dy) for dx in range(SIDE) for dy in range(SIDE) if dx or dy),
    key=lambda hop: -sum(min(d, SIDE - d) for d in hop),
)


def drawdown_kernel(n_tm, n_paths, returns_ref, w_ref, out_ref,
                    x, w_all, w_both, y, outbox, inbox,
                    x_sem, w_in_sem, w_send_sem, w_recv_sem, row_sem, send_sem, recv_sem):
    tm = lax.axis_index("tm")
    paths = lax.axis_index("paths")
    steps, n_local, assets = returns_ref.shape
    rows, port = w_ref.shape
    chunks = n_local // LANES
    half = steps // 2
    held = port // n_tm

    def column(j):
        return j + (paths <= j).astype(jnp.int32)

    def plane(dx, dy):
        return lax.rem(tm // SIDE + dx, SIDE) * SIDE + lax.rem(tm + dy, SIDE)

    barrier = pltpu.get_barrier_semaphore()
    for j in range(n_paths - 1):
        pl.semaphore_signal(barrier, inc=1, device_id=(tm, column(j)), device_id_type=MESH)
    for d in range(1, SIDE):
        pl.semaphore_signal(barrier, inc=1, device_id=(plane(d, 0), paths), device_id_type=MESH)
        pl.semaphore_signal(barrier, inc=1, device_id=(plane(0, d), paths), device_id_type=MESH)
    own_rows = pl.ds(pl.multiple_of(paths * rows, rows), rows)
    w_load = pltpu.make_async_copy(w_ref, w_all.at[own_rows, :], w_in_sem)
    w_load.start()
    x_load = pltpu.make_async_copy(returns_ref, x, x_sem)
    x_load.start()
    w_load.wait()

    pl.semaphore_wait(barrier, n_paths - 1 + 2 * (SIDE - 1))

    w_sends = []
    for j in range(n_paths - 1):
        copy = pltpu.make_async_remote_copy(
            src_ref=w_all.at[own_rows, :], dst_ref=w_all.at[own_rows, :],
            send_sem=w_send_sem.at[j], recv_sem=w_recv_sem.at[paths],
            device_id=(tm, column(j)), device_id_type=MESH)
        copy.start()
        w_sends.append(copy)
    for d in range(1, SIDE):
        pl.semaphore_signal(row_sem, inc=1, device_id=(plane(d, 0), paths), device_id_type=MESH)
    x_load.wait()
    pl.semaphore_wait(row_sem, SIDE - 1)
    for j in range(n_paths - 1):
        peer = column(j)
        rows_in = pl.ds(pl.multiple_of(peer * rows, rows), rows)
        pltpu.make_async_remote_copy(
            src_ref=w_all.at[rows_in, :], dst_ref=w_all.at[rows_in, :],
            send_sem=w_send_sem.at[j], recv_sem=w_recv_sem.at[peer],
            device_id=(tm, peer), device_id_type=MESH).wait_recv()

    source = lax.broadcasted_iota(jnp.int32, (port, LANES), 0)
    lane = lax.broadcasted_iota(jnp.int32, (port, LANES), 1)
    spread = jnp.where(source == (lane // SUB) * held + lane % held, 1.0, 0.0).astype(jnp.bfloat16)
    wide = jnp.dot(w_all[...], spread, preferred_element_type=jnp.float32)
    first = (lax.broadcasted_iota(jnp.int32, (assets, LANES), 1) % SUB) < held
    zeros = jnp.zeros((assets, LANES), jnp.bfloat16)
    for h, part in enumerate((jnp.where(first, wide, 0.0), jnp.where(first, 0.0, wide))):
        part = part.astype(jnp.bfloat16)
        for b in range(PAIR):
            rows_b = pl.ds((b * 2 + h) * assets, assets)
            for other in range(PAIR):
                w_both[rows_b, pl.ds(other * LANES, LANES)] = part if other == b else zeros

    second = (lax.broadcasted_iota(jnp.int32, (LANES, LANES), 1) % SUB) >= held
    group = 32
    sends = []
    for g in range(chunks // PAIR):
        for r in range(LANES // group):
            parts = [
                x[h * half:(h + 1) * half, pl.ds((g * PAIR + b) * LANES + r * group, group), :].reshape(half * group, assets)
                for b in range(PAIR) for h in range(2)
            ]
            y[g, r] = jnp.dot(jnp.concatenate(parts, axis=1), w_both[...], preferred_element_type=jnp.float32)
        for b in range(PAIR):
            c = g * PAIR + b
            lanes = pl.ds(b * LANES, LANES)
            total, high, low, deep = [], [], [], []
            for r in range(LANES // group):
                v = y[g, r, pl.ds(0, group), lanes]
                hi = jnp.maximum(v, 0.0)
                lo = jnp.minimum(v, 0.0)
                dd = hi - v
                for t in range(1, half):
                    v = v + y[g, r, pl.ds(t * group, group), lanes]
                    hi = jnp.maximum(hi, v)
                    lo = jnp.minimum(lo, v)
                    dd = jnp.maximum(dd, hi - v)
                total.append(v)
                high.append(hi)
                low.append(lo)
                deep.append(dd)
            total, high, low, deep = (jnp.concatenate(part, axis=0) for part in (total, high, low, deep))
            t0, h0, l0, d0 = (pltpu.roll(part, held, 1) for part in (total, high, low, deep))
            m_total = t0 + total
            m_high = jnp.maximum(h0, t0 + high)
            m_low = jnp.minimum(l0, t0 + low)
            m_deep = jnp.maximum(jnp.maximum(d0, deep), h0 - (t0 + low))
            th = jnp.where(second, m_high, pltpu.roll(m_total, LANES - held, 1))
            ld = jnp.where(second, m_deep, pltpu.roll(m_low, LANES - held, 1))
            outbox[c, :, 0] = th.T.reshape(n_tm, SUB, LANES)
            outbox[c, :, 1] = ld.T.reshape(n_tm, SUB, LANES)
            for j, hop in enumerate(HOPS):
                to = plane(*hop)
                copy = pltpu.make_async_remote_copy(
                    src_ref=outbox.at[c, to], dst_ref=inbox.at[c, tm],
                    send_sem=send_sem.at[c, j], recv_sem=recv_sem.at[c, tm],
                    device_id=(to, paths), device_id_type=MESH)
                copy.start()
                sends.append(copy)
            inbox[c, pl.ds(tm, 1)] = outbox[c, pl.ds(tm, 1)]

    for c in range(chunks):
        for j, hop in enumerate(HOPS):
            peer = plane(*hop)
            pltpu.make_async_remote_copy(
                src_ref=outbox.at[c, peer], dst_ref=inbox.at[c, peer],
                send_sem=send_sem.at[c, j], recv_sem=recv_sem.at[c, peer],
                device_id=(peer, paths), device_id_type=MESH).wait_recv()
        offset = jnp.zeros((SUB, LANES), jnp.float32)
        peak = jnp.zeros((SUB, LANES), jnp.float32)
        fall = jnp.zeros((SUB, LANES), jnp.float32)
        for s in range(n_tm):
            th = inbox[c, s, 0]
            ld = inbox[c, s, 1]
            fall = jnp.maximum(fall, jnp.maximum(pltpu.roll(ld, held, 0), peak - (offset + ld)))
            peak = jnp.maximum(peak, offset + pltpu.roll(th, held, 0))
            offset = offset + th
        out_ref[:, pl.ds(c * LANES, LANES)] = fall[:held]

    for copy in w_sends + sends:
        copy.wait_send()


def store_kernel(in_ref, out_ref, sem):
    copy = pltpu.make_async_copy(in_ref, out_ref, sem)
    copy.start()
    copy.wait()


def shards(returns, weights):
    n_tm, n_paths = lax.axis_size("tm"), lax.axis_size("paths")
    steps, n_local, assets = returns.shape
    rows, port = weights.shape
    chunks = n_local // LANES
    half = steps // 2
    held = port // n_tm
    f32, bf16 = jnp.float32, jnp.bfloat16
    vmem = pl.BlockSpec(memory_space=pltpu.VMEM)
    falls = pl.pallas_call(
        lambda *refs: drawdown_kernel(n_tm, n_paths, *refs),
        name="drawdown",
        out_shape=jax.ShapeDtypeStruct((held, n_local), f32),
        in_specs=[pl.BlockSpec(memory_space=pl.ANY)] * 2,
        out_specs=vmem,
        scratch_shapes=[
            pltpu.VMEM(returns.shape, bf16),
            pltpu.VMEM((assets, port), bf16),
            pltpu.VMEM((2 * PAIR * assets, PAIR * LANES), bf16),
            pltpu.VMEM((chunks // PAIR, LANES // 32, half * 32, PAIR * LANES), f32),
            pltpu.VMEM((chunks, n_tm, 2, SUB, LANES), f32),
            pltpu.VMEM((chunks, n_tm, 2, SUB, LANES), f32),
            pltpu.SemaphoreType.DMA,
            pltpu.SemaphoreType.DMA,
            pltpu.SemaphoreType.DMA((n_paths,)),
            pltpu.SemaphoreType.DMA((n_paths,)),
            pltpu.SemaphoreType.REGULAR,
            pltpu.SemaphoreType.DMA((chunks, n_tm)),
            pltpu.SemaphoreType.DMA((chunks, n_tm)),
        ],
        compiler_params=pltpu.CompilerParams(
            collective_id=0, has_side_effects=True, vmem_limit_bytes=44 * 1024 * 1024
        ),
    )(*(pltpu.with_memory_space_constraint(part, pltpu.HBM) for part in (returns, weights)))
    return pl.pallas_call(
        store_kernel,
        name="store",
        out_shape=jax.ShapeDtypeStruct((held, n_local), f32),
        in_specs=[vmem],
        out_specs=pl.BlockSpec(memory_space=pltpu.HBM),
        scratch_shapes=[pltpu.SemaphoreType.DMA],
        compiler_params=pltpu.CompilerParams(has_side_effects=True, vmem_limit_bytes=1024 * 1024),
    )(falls)


def solution(mesh):
    in_specs = (P("tm", "paths", None), P("paths", None))
    out_specs = P("tm", "paths")
    return jax.shard_map(shards, mesh=mesh, in_specs=in_specs, out_specs=out_specs, check_vma=False)
```

```python
import jax
import jax.numpy as jnp
from jax import lax
from jax.experimental import pallas as pl
from jax.experimental.pallas import tpu as pltpu
from jax.sharding import PartitionSpec as P

MESH = pl.DeviceIdType.MESH
LANES = 128
SUB = 8
SIDE = 4
PAIR = 2
AHEAD = 2
HOPS = sorted(
    ((dx, dy) for dx in range(SIDE) for dy in range(SIDE) if dx or dy),
    key=lambda hop: -sum(min(d, SIDE - d) for d in hop),
)


def drawdown_kernel(n_tm, n_paths, returns_ref, w_ref, out_ref,
                    x, w_in, w_all, w_both, y, outbox, inbox,
                    x_sem, w_in_sem, w_send_sem, w_recv_sem, row_sem, send_sem, recv_sem):
    tm = lax.axis_index("tm")
    paths = lax.axis_index("paths")
    steps, n_local, assets = returns_ref.shape
    rows, port = w_ref.shape
    chunks = n_local // LANES
    half = steps // 2
    held = port // n_tm

    def column(j):
        return j + (paths <= j).astype(jnp.int32)

    def plane(dx, dy):
        return lax.rem(tm // SIDE + dx, SIDE) * SIDE + lax.rem(tm + dy, SIDE)

    barrier = pltpu.get_barrier_semaphore()
    for j in range(n_paths - 1):
        pl.semaphore_signal(barrier, inc=1, device_id=(tm, column(j)), device_id_type=MESH)
    for d in range(1, SIDE):
        pl.semaphore_signal(barrier, inc=1, device_id=(plane(d, 0), paths), device_id_type=MESH)
        pl.semaphore_signal(barrier, inc=1, device_id=(plane(0, d), paths), device_id_type=MESH)
    w_load = pltpu.make_async_copy(w_ref, w_in, w_in_sem)
    w_load.start()
    x_load = pltpu.make_async_copy(returns_ref, x, x_sem)
    x_load.start()

    source = lax.broadcasted_iota(jnp.int32, (port, LANES), 0)
    lane = lax.broadcasted_iota(jnp.int32, (port, LANES), 1)
    spread = jnp.where(source == (lane // SUB) * held + lane % held, 1.0, 0.0).astype(jnp.bfloat16)
    own_rows = pl.ds(pl.multiple_of(paths * rows, rows), rows)
    w_load.wait()
    w_all[own_rows, :] = jnp.dot(w_in[...], spread, preferred_element_type=jnp.float32).astype(jnp.bfloat16)

    first = (lax.broadcasted_iota(jnp.int32, (rows, LANES), 1) % SUB) < held
    w_both[...] = jnp.zeros_like(w_both)

    def lay_out(source):
        wide = w_all[pl.ds(pl.multiple_of(source * rows, rows), rows), :].astype(jnp.float32)
        for h, part in enumerate((jnp.where(first, wide, 0.0), jnp.where(first, 0.0, wide))):
            part = part.astype(jnp.bfloat16)
            for b in range(PAIR):
                at = pl.multiple_of((b * 2 + h) * assets + source * rows, rows)
                w_both[pl.ds(at, rows), pl.ds(b * LANES, LANES)] = part

    lay_out(paths)
    pl.semaphore_wait(barrier, n_paths - 1 + 2 * (SIDE - 1))

    w_sends = []
    for j in range(n_paths - 1):
        copy = pltpu.make_async_remote_copy(
            src_ref=w_all.at[own_rows, :], dst_ref=w_all.at[own_rows, :],
            send_sem=w_send_sem.at[j], recv_sem=w_recv_sem.at[paths],
            device_id=(tm, column(j)), device_id_type=MESH)
        copy.start()
        w_sends.append(copy)
    for d in range(1, SIDE):
        pl.semaphore_signal(row_sem, inc=1, device_id=(plane(d, 0), paths), device_id_type=MESH)
    x_load.wait()
    pl.semaphore_wait(row_sem, SIDE - 1)
    for j in range(n_paths - 1):
        peer = column(j)
        rows_in = pl.ds(pl.multiple_of(peer * rows, rows), rows)
        pltpu.make_async_remote_copy(
            src_ref=w_all.at[rows_in, :], dst_ref=w_all.at[rows_in, :],
            send_sem=w_send_sem.at[j], recv_sem=w_recv_sem.at[peer],
            device_id=(tm, peer), device_id_type=MESH).wait_recv()
        lay_out(peer)

    second = (lax.broadcasted_iota(jnp.int32, (LANES, LANES), 1) % SUB) >= held
    group = 32
    sends = []
    targets = [plane(*hop) for hop in HOPS]
    targets = [jnp.where(tm == 0, targets[0], 0)] + [jnp.where(to == 0, targets[0], to) for to in targets[1:]]
    def multiply(g, which):
        for r in which:
            parts = [
                x[h * half:(h + 1) * half, pl.ds((g * PAIR + b) * LANES + r * group, group), :].reshape(half * group, assets)
                for b in range(PAIR) for h in range(2)
            ]
            y[g, r] = jnp.dot(jnp.concatenate(parts, axis=1), w_both[...], preferred_element_type=jnp.float32)

    groups = LANES // group
    multiply(0, range(groups))
    for g in range(chunks // PAIR):
        if g + 1 < chunks // PAIR:
            multiply(g + 1, range(AHEAD))
        for b in range(PAIR):
            lanes = pl.ds(b * LANES, LANES)
            total, high, low, deep = [], [], [], []
            for r in range(LANES // group):
                v = y[g, r, pl.ds(0, group), lanes]
                hi = jnp.maximum(v, 0.0)
                lo = jnp.minimum(v, 0.0)
                dd = hi - v
                for t in range(1, half):
                    v = v + y[g, r, pl.ds(t * group, group), lanes]
                    hi = jnp.maximum(hi, v)
                    lo = jnp.minimum(lo, v)
                    dd = jnp.maximum(dd, hi - v)
                total.append(v)
                high.append(hi)
                low.append(lo)
                deep.append(dd)
            total, high, low, deep = (jnp.concatenate(part, axis=0) for part in (total, high, low, deep))
            t0, h0, l0, d0 = (pltpu.roll(part, held, 1) for part in (total, high, low, deep))
            m_total = t0 + total
            m_high = jnp.maximum(h0, t0 + high)
            m_low = jnp.minimum(l0, t0 + low)
            m_deep = jnp.maximum(jnp.maximum(d0, deep), h0 - (t0 + low))
            th = jnp.where(second, m_high, pltpu.roll(m_total, LANES - held, 1))
            ld = jnp.where(second, m_deep, pltpu.roll(m_low, LANES - held, 1))
            outbox[g, :, b, 0] = th.T.reshape(n_tm, SUB, LANES)
            outbox[g, :, b, 1] = ld.T.reshape(n_tm, SUB, LANES)
        for to in targets:
            copy = pltpu.make_async_remote_copy(
                src_ref=outbox.at[g, to], dst_ref=inbox.at[g, tm],
                send_sem=send_sem.at[g, to], recv_sem=recv_sem.at[g, tm],
                device_id=(to, paths), device_id_type=MESH)
            copy.start()
            sends.append(copy)
        inbox[g, pl.ds(tm, 1)] = outbox[g, pl.ds(tm, 1)]
        if g + 1 < chunks // PAIR:
            multiply(g + 1, range(AHEAD, groups))

    for g in range(chunks // PAIR):
        for hop in HOPS:
            peer = plane(*hop)
            pltpu.make_async_remote_copy(
                src_ref=outbox.at[g, peer], dst_ref=inbox.at[g, peer],
                send_sem=send_sem.at[g, peer], recv_sem=recv_sem.at[g, peer],
                device_id=(peer, paths), device_id_type=MESH).wait_recv()
        offset = peak = fall = jnp.zeros((PAIR, SUB, LANES), jnp.float32)
        for s in range(n_tm):
            th = inbox[g, s, :, 0]
            ld = inbox[g, s, :, 1]
            fall = jnp.maximum(fall, jnp.maximum(pltpu.roll(ld, held, 1), peak - (offset + ld)))
            peak = jnp.maximum(peak, offset + pltpu.roll(th, held, 1))
            offset = offset + th
        for b in range(PAIR):
            out_ref[:, pl.ds((g * PAIR + b) * LANES, LANES)] = fall[b, :held]

    for copy in w_sends + sends:
        copy.wait_send()


def store_kernel(in_ref, out_ref, sem):
    copy = pltpu.make_async_copy(in_ref, out_ref, sem)
    copy.start()
    copy.wait()


def shards(returns, weights):
    n_tm, n_paths = lax.axis_size("tm"), lax.axis_size("paths")
    steps, n_local, assets = returns.shape
    rows, port = weights.shape
    chunks = n_local // LANES
    half = steps // 2
    held = port // n_tm
    f32, bf16 = jnp.float32, jnp.bfloat16
    vmem = pl.BlockSpec(memory_space=pltpu.VMEM)
    falls = pl.pallas_call(
        lambda *refs: drawdown_kernel(n_tm, n_paths, *refs),
        name="drawdown",
        out_shape=jax.ShapeDtypeStruct((held, n_local), f32),
        in_specs=[pl.BlockSpec(memory_space=pl.ANY)] * 2,
        out_specs=vmem,
        scratch_shapes=[
            pltpu.VMEM(returns.shape, bf16),
            pltpu.VMEM((rows, port), bf16),
            pltpu.VMEM((assets, LANES), bf16),
            pltpu.VMEM((2 * PAIR * assets, PAIR * LANES), bf16),
            pltpu.VMEM((chunks // PAIR, LANES // 32, half * 32, PAIR * LANES), f32),
            pltpu.VMEM((chunks // PAIR, n_tm, PAIR, 2, SUB, LANES), f32),
            pltpu.VMEM((chunks // PAIR, n_tm, PAIR, 2, SUB, LANES), f32),
            pltpu.SemaphoreType.DMA,
            pltpu.SemaphoreType.DMA,
            pltpu.SemaphoreType.DMA((n_paths,)),
            pltpu.SemaphoreType.DMA((n_paths,)),
            pltpu.SemaphoreType.REGULAR,
            pltpu.SemaphoreType.DMA((chunks // PAIR, n_tm)),
            pltpu.SemaphoreType.DMA((chunks // PAIR, n_tm)),
        ],
        compiler_params=pltpu.CompilerParams(
            collective_id=0, has_side_effects=True, vmem_limit_bytes=44 * 1024 * 1024
        ),
    )(*(pltpu.with_memory_space_constraint(part, pltpu.HBM) for part in (returns, weights)))
    return pl.pallas_call(
        store_kernel,
        name="store",
        out_shape=jax.ShapeDtypeStruct((held, n_local), f32),
        in_specs=[vmem],
        out_specs=pl.BlockSpec(memory_space=pltpu.HBM),
        scratch_shapes=[pltpu.SemaphoreType.DMA],
        compiler_params=pltpu.CompilerParams(has_side_effects=True, vmem_limit_bytes=1024 * 1024),
    )(falls)


def solution(mesh):
    in_specs = (P("tm", "paths", None), P("paths", None))
    out_specs = P("tm", "paths")
    return jax.shard_map(shards, mesh=mesh, in_specs=in_specs, out_specs=out_specs, check_vma=False)
```

```python
import jax
import jax.numpy as jnp
from jax import lax
from jax.experimental import pallas as pl
from jax.experimental.pallas import tpu as pltpu
from jax.sharding import PartitionSpec as P

MESH = pl.DeviceIdType.MESH
LANES = 128
SUB = 8
SIDE = 4
PAIR = 2
AHEAD = 2
HOPS = sorted(
    ((dx, dy) for dx in range(SIDE) for dy in range(SIDE) if dx or dy),
    key=lambda hop: -sum(min(d, SIDE - d) for d in hop),
)


def drawdown_kernel(n_tm, n_paths, returns_ref, w_ref, out_ref,
                    x, w_in, w_all, w_both, y, outbox, inbox,
                    x_sem, w_in_sem, w_send_sem, w_recv_sem, late_sem, row_sem, send_sem, recv_sem):
    tm = lax.axis_index("tm")
    paths = lax.axis_index("paths")
    steps, n_local, assets = returns_ref.shape
    rows, port = w_ref.shape
    chunks = n_local // LANES
    half = steps // 2
    held = port // n_tm

    def column(j):
        return j + (paths <= j).astype(jnp.int32)

    def plane(dx, dy):
        return lax.rem(tm // SIDE + dx, SIDE) * SIDE + lax.rem(tm + dy, SIDE)

    barrier = pltpu.get_barrier_semaphore()
    late = paths >= n_paths // 2
    for j in range(n_paths - 1):
        to = column(j)

        @pl.when(jnp.logical_not(jnp.logical_and(late, to < n_paths // 2)))
        def _(to=to):
            pl.semaphore_signal(barrier, inc=1, device_id=(tm, to), device_id_type=MESH)
    for d in range(1, SIDE):
        pl.semaphore_signal(barrier, inc=1, device_id=(plane(d, 0), paths), device_id_type=MESH)
        pl.semaphore_signal(barrier, inc=1, device_id=(plane(0, d), paths), device_id_type=MESH)
    w_load = pltpu.make_async_copy(w_ref, w_in, w_in_sem)
    w_load.start()
    x_load = pltpu.make_async_copy(returns_ref, x, x_sem)
    x_load.start()

    source = lax.broadcasted_iota(jnp.int32, (port, LANES), 0)
    lane = lax.broadcasted_iota(jnp.int32, (port, LANES), 1)
    spread = jnp.where(source == (lane // SUB) * held + lane % held, 1.0, 0.0).astype(jnp.bfloat16)
    own_rows = pl.ds(pl.multiple_of(paths * rows, rows), rows)
    w_load.wait()
    w_all[own_rows, :] = jnp.dot(w_in[...], spread, preferred_element_type=jnp.float32).astype(jnp.bfloat16)

    team = n_paths // 2
    mine = paths // team
    depth = team * rows
    first = (lax.broadcasted_iota(jnp.int32, (rows, LANES), 1) % SUB) < held
    w_both[...] = jnp.zeros_like(w_both)

    def lay_out(source, stage):
        wide = w_all[pl.ds(pl.multiple_of(source * rows, rows), rows), :].astype(jnp.float32)
        for h, part in enumerate((jnp.where(first, wide, 0.0), jnp.where(first, 0.0, wide))):
            part = part.astype(jnp.bfloat16)
            for b in range(PAIR):
                at = pl.multiple_of((b * 2 + h) * depth + lax.rem(source, team) * rows, rows)
                w_both[stage, pl.ds(at, rows), pl.ds(b * LANES, LANES)] = part

    lay_out(paths, 0)
    pl.semaphore_wait(barrier, n_paths // 2 - 1 + 2 * (SIDE - 1) + late.astype(jnp.int32) * (n_paths // 2))

    own_team = [mine * team + j + (lax.rem(paths, team) <= j).astype(jnp.int32) for j in range(team - 1)]
    other_team = [(1 - mine) * team + j for j in range(team)]

    def carry(source, to):
        at = pl.ds(pl.multiple_of(source * rows, rows), rows)
        return pltpu.make_async_remote_copy(
            src_ref=w_all.at[at, :], dst_ref=w_all.at[at, :],
            send_sem=w_send_sem.at[to], recv_sem=w_recv_sem.at[source],
            device_id=(tm, to), device_id_type=MESH)

    to_own = [carry(paths, to) for to in own_team]
    to_other = [carry(paths, to) for to in other_team]
    @pl.when(late)
    def _():
        for to in other_team:
            pl.semaphore_signal(late_sem, inc=1, device_id=(tm, to), device_id_type=MESH)
        for copy in to_other:
            copy.start()

    for copy in to_own:
        copy.start()
    w_sends = to_own + to_other
    for d in range(1, SIDE):
        pl.semaphore_signal(row_sem, inc=1, device_id=(plane(d, 0), paths), device_id_type=MESH)
    second = (lax.broadcasted_iota(jnp.int32, (LANES, LANES), 1) % SUB) >= held
    group = 32
    sends = []
    targets = [plane(*hop) for hop in HOPS]
    targets = [jnp.where(tm == 0, targets[0], 0)] + [jnp.where(to == 0, targets[0], to) for to in targets[1:]]
    def multiply(stage, g, which):
        side = mine if stage == 0 else 1 - mine
        columns = pl.ds(pl.multiple_of(side * depth, depth), depth)
        for r in which:
            parts = [
                x[h * half:(h + 1) * half, pl.ds((g * PAIR + b) * LANES + r * group, group), columns].reshape(half * group, depth)
                for b in range(PAIR) for h in range(2)
            ]
            share = jnp.dot(jnp.concatenate(parts, axis=1), w_both[stage], preferred_element_type=jnp.float32)
            y[g, r] = share if stage == 0 else y[g, r] + share

    groups = LANES // group
    for peer in own_team:
        carry(peer, peer).wait_recv()
        lay_out(peer, 0)
    x_load.wait()
    for g in range(chunks // PAIR):
        multiply(0, g, range(groups))

    @pl.when(jnp.logical_not(late))
    def _():
        pl.semaphore_wait(late_sem, team)
        for copy in to_other:
            copy.start()

    for peer in other_team:
        carry(peer, peer).wait_recv()
        lay_out(peer, 1)
    multiply(1, 0, range(groups))
    for g in range(chunks // PAIR):
        if g + 1 < chunks // PAIR:
            multiply(1, g + 1, range(AHEAD))
        for b in range(PAIR):
            lanes = pl.ds(b * LANES, LANES)
            total, high, low, deep = [], [], [], []
            for r in range(LANES // group):
                v = y[g, r, pl.ds(0, group), lanes]
                hi = jnp.maximum(v, 0.0)
                lo = jnp.minimum(v, 0.0)
                dd = hi - v
                for t in range(1, half):
                    v = v + y[g, r, pl.ds(t * group, group), lanes]
                    hi = jnp.maximum(hi, v)
                    lo = jnp.minimum(lo, v)
                    dd = jnp.maximum(dd, hi - v)
                total.append(v)
                high.append(hi)
                low.append(lo)
                deep.append(dd)
            total, high, low, deep = (jnp.concatenate(part, axis=0) for part in (total, high, low, deep))
            t0, h0, l0, d0 = (pltpu.roll(part, held, 1) for part in (total, high, low, deep))
            m_total = t0 + total
            m_high = jnp.maximum(h0, t0 + high)
            m_low = jnp.minimum(l0, t0 + low)
            m_deep = jnp.maximum(jnp.maximum(d0, deep), h0 - (t0 + low))
            th = jnp.where(second, m_high, pltpu.roll(m_total, LANES - held, 1))
            ld = jnp.where(second, m_deep, pltpu.roll(m_low, LANES - held, 1))
            outbox[g, :, b, 0] = th.T.reshape(n_tm, SUB, LANES)
            outbox[g, :, b, 1] = ld.T.reshape(n_tm, SUB, LANES)
        if g == 0:
            pl.semaphore_wait(row_sem, SIDE - 1)
        for to in targets:
            copy = pltpu.make_async_remote_copy(
                src_ref=outbox.at[g, to], dst_ref=inbox.at[g, tm],
                send_sem=send_sem.at[g, to], recv_sem=recv_sem.at[g, tm],
                device_id=(to, paths), device_id_type=MESH)
            copy.start()
            sends.append(copy)
        inbox[g, pl.ds(tm, 1)] = outbox[g, pl.ds(tm, 1)]
        if g + 1 < chunks // PAIR:
            multiply(1, g + 1, range(AHEAD, groups))

    for g in range(chunks // PAIR):
        for hop in HOPS:
            peer = plane(*hop)
            pltpu.make_async_remote_copy(
                src_ref=outbox.at[g, peer], dst_ref=inbox.at[g, peer],
                send_sem=send_sem.at[g, peer], recv_sem=recv_sem.at[g, peer],
                device_id=(peer, paths), device_id_type=MESH).wait_recv()
        offset = peak = fall = jnp.zeros((PAIR, SUB, LANES), jnp.float32)
        for s in range(n_tm):
            th = inbox[g, s, :, 0]
            ld = inbox[g, s, :, 1]
            fall = jnp.maximum(fall, jnp.maximum(pltpu.roll(ld, held, 1), peak - (offset + ld)))
            peak = jnp.maximum(peak, offset + pltpu.roll(th, held, 1))
            offset = offset + th
        for b in range(PAIR):
            out_ref[:, pl.ds((g * PAIR + b) * LANES, LANES)] = fall[b, :held]

    for copy in w_sends + sends:
        copy.wait_send()


def store_kernel(in_ref, out_ref, sem):
    copy = pltpu.make_async_copy(in_ref, out_ref, sem)
    copy.start()
    copy.wait()


def shards(returns, weights):
    n_tm, n_paths = lax.axis_size("tm"), lax.axis_size("paths")
    steps, n_local, assets = returns.shape
    rows, port = weights.shape
    chunks = n_local // LANES
    half = steps // 2
    held = port // n_tm
    f32, bf16 = jnp.float32, jnp.bfloat16
    vmem = pl.BlockSpec(memory_space=pltpu.VMEM)
    falls = pl.pallas_call(
        lambda *refs: drawdown_kernel(n_tm, n_paths, *refs),
        name="drawdown",
        out_shape=jax.ShapeDtypeStruct((held, n_local), f32),
        in_specs=[pl.BlockSpec(memory_space=pl.ANY)] * 2,
        out_specs=vmem,
        scratch_shapes=[
            pltpu.VMEM(returns.shape, bf16),
            pltpu.VMEM((rows, port), bf16),
            pltpu.VMEM((assets, LANES), bf16),
            pltpu.VMEM((2, PAIR * assets, PAIR * LANES), bf16),
            pltpu.VMEM((chunks // PAIR, LANES // 32, half * 32, PAIR * LANES), f32),
            pltpu.VMEM((chunks // PAIR, n_tm, PAIR, 2, SUB, LANES), f32),
            pltpu.VMEM((chunks // PAIR, n_tm, PAIR, 2, SUB, LANES), f32),
            pltpu.SemaphoreType.DMA,
            pltpu.SemaphoreType.DMA,
            pltpu.SemaphoreType.DMA((n_paths,)),
            pltpu.SemaphoreType.DMA((n_paths,)),
            pltpu.SemaphoreType.REGULAR,
            pltpu.SemaphoreType.REGULAR,
            pltpu.SemaphoreType.DMA((chunks // PAIR, n_tm)),
            pltpu.SemaphoreType.DMA((chunks // PAIR, n_tm)),
        ],
        compiler_params=pltpu.CompilerParams(
            collective_id=0, has_side_effects=True, vmem_limit_bytes=44 * 1024 * 1024
        ),
    )(*(pltpu.with_memory_space_constraint(part, pltpu.HBM) for part in (returns, weights)))
    return pl.pallas_call(
        store_kernel,
        name="store",
        out_shape=jax.ShapeDtypeStruct((held, n_local), f32),
        in_specs=[vmem],
        out_specs=pl.BlockSpec(memory_space=pltpu.HBM),
        scratch_shapes=[pltpu.SemaphoreType.DMA],
        compiler_params=pltpu.CompilerParams(has_side_effects=True, vmem_limit_bytes=1024 * 1024),
    )(falls)


def solution(mesh):
    in_specs = (P("tm", "paths", None), P("paths", None))
    out_specs = P("tm", "paths")
    return jax.shard_map(shards, mesh=mesh, in_specs=in_specs, out_specs=out_specs, check_vma=False)
```
